32 devices in a mesh: head: 4 (over z), outer: 4 (over x, core), inner: 2 (over y).
Axes of the slice: x: 2, y: 2, z: 4, core: 2. Of those that a mesh axis runs over, the one named last changes fastest.
Arguments:
- query_nope: bfloat16 [1024, 2048], P(('outer', 'inner'), 'head'), may hold values from -6 to 6
- query_rope: bfloat16 [1024, 1024], P(('outer', 'inner'), 'head'), may hold values from -8 to 8
- cache: bfloat16 [1024, 576], P(('outer', 'inner')), may hold values from -8 to 8
- span_ids: int32 [16], P(('outer', 'inner')), may hold values from 0 to 15, as said below
- key_up: bfloat16 [512, 2048], P(None, 'head'), may hold values from -0.25 to 0.25
- value_up: bfloat16 [512, 2048], P(None, 'head'), may hold values from -1.5 to 1.5
- out_proj: bfloat16 [2048, 2048], P('head'), may hold values from -1.1953125 to 1.1953125
Outputs:
- mixed: bfloat16 [1024, 2048], P(('outer', 'inner'), 'head')
The draws below stay inside these ranges and needn't reach their ends.
Inputs may be any that keep to these rules, and one draw needn't show every extreme that they name: `span_ids`: each of 0 to 15 appears once; entries 2 r and 2 r + 1 belong to storage rows r * 128 to (r + 1) * 128 - 1.
All inputs are finite; a program needn't handle non-finite values.
Results may differ from the reference program's by a relative error of at most 0.014.
Values may be sent and summed in bfloat16 or wider, within the bound.
No kernel may reach another device: no remote copies, remote signals or barrier semaphores. Data moves between devices by JAX's collectives and lax.ppermute only.
A program may use at most 64 MiB of HBM per device.

```python
import math
import jax
import jax.numpy as jnp
from jax import lax

HEADS = 16
LATENT = 512
ROPE = 64
NOPE = 128
VDIM = 128
MODEL = 2048
SPAN = 64
SPANS = 16
SEQ = 1024


def span_order(key):
    return jax.random.permutation(jax.random.fold_in(key, 7), SPANS).astype(jnp.int32)


def draw_span_ids(key, part):
    return span_order(key)


def draw_cache(key, part):
    values_all = jax.random.normal(jax.random.fold_in(key, 1), (SEQ, LATENT + ROPE), jnp.float32)
    return jnp.clip(values_all, -8.0, 8.0).astype(jnp.bfloat16)


def draw_query_rope(key, part):
    values_all = jax.random.normal(jax.random.fold_in(key, 3), (SEQ, HEADS * ROPE), jnp.float32)
    return jnp.clip(values_all, -8.0, 8.0).astype(jnp.bfloat16)


def block_levels(rng, shape, split, least, high):
    level, own = 1.0, jax.random.fold_in(rng, 6)
    for dim, blocks in split:
        draws = jnp.exp(jax.random.uniform(jax.random.fold_in(own, dim), (blocks,), jnp.float32, least / len(split), high / len(split)))
        level = level * jnp.repeat(draws, shape[dim] // blocks).reshape([-1 if axis == dim else 1 for axis in range(len(shape))])
    return level


def scatter_about(stream_key, shape, width, reach, pieces=(), kind=jnp.bfloat16):
    drawn = width * jax.random.normal(stream_key, shape, jnp.float32)
    if pieces:
        drawn = drawn * block_levels(stream_key, shape, pieces, -0.22, 0.18)
    return jnp.clip(drawn, -reach, reach).astype(kind)


def setup_inputs(seed: int = 0) -> dict:
    key_of = jax.random.split(jax.random.key(seed), 8)
    return {
        "query_nope": scatter_about(key_of[0], (SEQ, HEADS * NOPE), 1.0, 6.0, ((0, 8), (1, 4))),
        "query_rope": draw_query_rope(jax.random.fold_in(key_of[7], 71), 0),
        "cache": draw_cache(jax.random.fold_in(key_of[7], 71), 0),
        "span_ids": draw_span_ids(jax.random.fold_in(key_of[7], 71), 0),
        "key_up": scatter_about(key_of[4], (LATENT, HEADS * NOPE), LATENT ** -0.5, 0.25, ((1, 4),)),
        "value_up": scatter_about(key_of[5], (LATENT, HEADS * VDIM), 0.25, 1.5, ((1, 4),)),
        "out_proj": scatter_about(key_of[6], (HEADS * VDIM, MODEL), 0.2, 1.1953125, ((0, 4),)),
    }


def reference(query_nope, query_rope, cache, span_ids, key_up, value_up, out_proj):
    seq_total = cache.shape[0]
    row_ids = jnp.arange(seq_total, dtype=jnp.int32)
    position = span_ids[row_ids // SPAN] * SPAN + row_ids % SPAN
    query_heads = query_nope.reshape(seq_total, HEADS, NOPE).astype(jnp.float32)
    key_weight = key_up.reshape(LATENT, HEADS, NOPE).astype(jnp.float32)
    q_latent = jnp.einsum("shd,chd->hsc", query_heads, key_weight).astype(jnp.bfloat16)
    q_rotary = jnp.transpose(query_rope.reshape(seq_total, HEADS, ROPE), (1, 0, 2))
    queries = jnp.concatenate([q_latent, q_rotary], axis=2).astype(jnp.float32)
    keys_all = cache.astype(jnp.float32)
    latent_all = keys_all[:, :LATENT]
    value_weight = value_up.reshape(LATENT, HEADS, VDIM).astype(jnp.float32)
    softmax_scale = (NOPE + ROPE) ** -0.5
    block_rows = math.gcd(seq_total, 512)

    def one_block(which_block):
        first_row = which_block * block_rows
        query_block = lax.dynamic_slice_in_dim(queries, first_row, block_rows, 1)
        query_pos = lax.dynamic_slice_in_dim(position, first_row, block_rows, 0)
        scores = jnp.einsum("hsc,tc->hst", query_block, keys_all) * softmax_scale
        visible = position[None, None, :] <= query_pos[None, :, None]
        scores = jnp.where(visible, scores, -jnp.inf)
        row_max = jnp.max(scores, axis=2, keepdims=True)
        expsum = jnp.exp(scores - row_max)
        denom = jnp.sum(expsum, axis=2)
        weights = lax.optimization_barrier(expsum.astype(jnp.bfloat16)).astype(jnp.float32)
        latent_out = jnp.einsum("hst,tc->hsc", weights, latent_all) / denom[:, :, None]
        latent_out = lax.optimization_barrier(latent_out.astype(jnp.bfloat16)).astype(jnp.float32)
        head_out = jnp.einsum("hsc,chd->shd", latent_out, value_weight)
        head_out = head_out.astype(jnp.bfloat16).reshape(block_rows, HEADS * VDIM)
        mixed = jnp.dot(head_out, out_proj, preferred_element_type=jnp.float32)
        return mixed.astype(jnp.bfloat16)

    blocks = lax.map(one_block, jnp.arange(seq_total // block_rows, dtype=jnp.int32))
    return blocks.reshape(seq_total, MODEL)
```

```python
import functools

import jax
import jax.numpy as jnp
from jax import lax
from jax.experimental import pallas as pl
from jax.experimental.pallas import tpu as pltpu
from jax.sharding import PartitionSpec as P

LATENT = 512
ROPE = 64
NOPE = 128
VDIM = 128
SPAN = 64
TAG = 16

lowest_start = -1e30
log2e = 1.4426950408889634
soft_scale = (NOPE + ROPE) ** (-0.5)
VMEM_BYTES = 24 * 1024 * 1024
NT = (((1,), (1,)), ((), ()))
TOKENS = ("outer", "inner")


def vmem():
    return pl.BlockSpec(memory_space=pltpu.VMEM)


def smem():
    return pl.BlockSpec(memory_space=pltpu.SMEM)


def call(body, out_shape, n_scalar, args, flops, scratch=()):
    return pl.pallas_call(
        body,
        out_shape=out_shape,
        in_specs=[smem()] * n_scalar + [vmem()] * (len(args) - n_scalar),
        out_specs=jax.tree.map(lambda _: vmem(), out_shape),
        scratch_shapes=list(scratch),
        compiler_params=pltpu.CompilerParams(vmem_limit_bytes=VMEM_BYTES),
        cost_estimate=pl.CostEstimate(flops=flops, bytes_accessed=1 << 20, transcendentals=0),
    )(*args)


def build_queries(heads, nope_ref, rope_ref, key_up_ref, out_ref):
    rows = nope_ref.shape[0]
    for h in range(heads):
        here = slice(h * rows, (h + 1) * rows)
        latent = lax.dot_general(
            nope_ref[:, h * NOPE : (h + 1) * NOPE],
            key_up_ref[:, h * NOPE : (h + 1) * NOPE],
            NT,
            preferred_element_type=jnp.float32,
        )
        out_ref[here, :LATENT] = latent.astype(jnp.bfloat16)
        out_ref[here, LATENT : LATENT + ROPE] = rope_ref[:, h * ROPE : (h + 1) * ROPE]


def gather_keys(shards, keys):
    at = 0
    for ref in shards:
        keys[:, at : at + ref.shape[1]] = ref[...]
        at += ref.shape[1]


def positions(ids_ref, heads, rows):
    row = lax.broadcasted_iota(jnp.int32, (rows, 1), 0)
    pos = row % SPAN
    for k in range(rows // SPAN):
        pos = pos + jnp.where(row // SPAN == k, ids_ref[k] * SPAN, 0)
    return pos.astype(jnp.float32)


def scores_of(q, keys, row_pos):
    width = keys.shape[1]
    s = jnp.dot(q, keys[: LATENT + ROPE, :], preferred_element_type=jnp.float32)
    tag = keys[LATENT + ROPE : LATENT + ROPE + TAG, :][:1].astype(jnp.float32)
    lane = lax.broadcasted_iota(jnp.int32, (1, width), 1) % SPAN
    key_pos = tag * SPAN + lane.astype(jnp.float32)
    return jnp.where(key_pos <= row_pos, s, -jnp.inf)


def attend(heads, n_shards, first, ids_ref, q_ref, *refs):
    shards = refs[:n_shards]
    if first:
        m_ref, l_ref, acc_ref, keys = refs[n_shards:]
    else:
        m_in, l_in, acc_in, m_ref, l_ref, acc_ref, keys = refs[n_shards:]
    rows = q_ref.shape[0] // heads
    gather_keys(shards, keys)
    row_pos = positions(ids_ref, heads, rows)
    for h in range(heads):
        here = slice(h * rows, (h + 1) * rows)
        s = scores_of(q_ref[here, :], keys, row_pos)
        m = jnp.maximum(jnp.max(s, axis=1, keepdims=True), lowest_start)
        if not first:
            old = m_in[here, :1]
            m = jnp.maximum(m, old)
        w = jnp.exp2((s - m) * (soft_scale * log2e))
        l = jnp.sum(w, axis=1, keepdims=True)
        acc = lax.dot_general(
            w.astype(jnp.bfloat16), keys[:LATENT, :], NT, preferred_element_type=jnp.float32
        )
        if not first:
            again = jnp.exp2((old - m) * (soft_scale * log2e))
            l = l + l_in[here, :1] * again
            acc = acc + acc_in[here, :] * again
        m_ref[here, :] = jnp.broadcast_to(m, (rows, 128))
        l_ref[here, :] = jnp.broadcast_to(l, (rows, 128))
        acc_ref[here, :] = acc


def finish(heads, n_shards, parts, ids_ref, where_ref, q_ref, *refs):
    shards = refs[:n_shards]
    m_in, l_in, acc_in, value_ref, proj_ref = refs[n_shards : n_shards + 5]
    outs = refs[n_shards + 5 : n_shards + 5 + parts]
    keys, head_out = refs[n_shards + 5 + parts :]
    rows = q_ref.shape[0] // heads
    gather_keys(shards, keys)
    row_pos = positions(ids_ref, heads, rows)
    for h in range(heads):
        here = slice(h * rows, (h + 1) * rows)
        s = scores_of(q_ref[here, :], keys, row_pos)
        old = m_in[here, :1]
        m = jnp.maximum(jnp.max(s, axis=1, keepdims=True), old)
        w = jnp.exp2((s - m) * (soft_scale * log2e))
        again = jnp.exp2((old - m) * (soft_scale * log2e))
        l = jnp.sum(w, axis=1, keepdims=True) + l_in[here, :1] * again
        acc = lax.dot_general(
            w.astype(jnp.bfloat16), keys[:LATENT, :], NT, preferred_element_type=jnp.float32
        )
        latent = ((acc + acc_in[here, :] * again) / l).astype(jnp.bfloat16)
        head_out[:, h * VDIM : (h + 1) * VDIM] = jnp.dot(
            latent, value_ref[:, h * VDIM : (h + 1) * VDIM], preferred_element_type=jnp.float32
        ).astype(jnp.bfloat16)
    width = proj_ref.shape[1] // parts
    for k in range(parts):
        at = pl.multiple_of(where_ref[k] * width, 128)
        outs[k][...] = jnp.dot(
            head_out[...], proj_ref[:, pl.ds(at, width)], preferred_element_type=jnp.float32
        ).astype(outs[k].dtype)


def add_parts(*refs):
    total = refs[0][...].astype(jnp.float32)
    for ref in refs[1:-1]:
        total = total + ref[...].astype(jnp.float32)
    refs[-1][...] = total.astype(jnp.bfloat16)


def swap(a, axes, n, flip):
    return lax.ppermute(a, axes, [(i, flip(i)) for i in range(n)])


def shards(sizes, query_nope, query_rope, cache, span_ids, key_up, value_up, out_proj):
    head_n, outer_n, inner_n = sizes
    rows = cache.shape[0]
    heads = key_up.shape[1] // NOPE
    total_rows = heads * rows
    f32 = jnp.float32
    width = LATENT + ROPE + TAG
    tag = jnp.broadcast_to(
        jnp.repeat(span_ids, SPAN, total_repeat_length=rows)[None, :], (TAG, rows)
    ).astype(jnp.bfloat16)
    own = jnp.concatenate([cache.T, tag], axis=0)
    n = outer_n * inner_n
    core, step = inner_n, 2 * inner_n
    state_shape = (
        jax.ShapeDtypeStruct((total_rows, 128), f32),
        jax.ShapeDtypeStruct((total_rows, 128), f32),
        jax.ShapeDtypeStruct((total_rows, LATENT), f32),
    )

    queries = call(
        functools.partial(build_queries, heads),
        jax.ShapeDtypeStruct((total_rows, LATENT + ROPE), jnp.bfloat16),
        0,
        (query_nope, query_rope, key_up),
        2 * rows * NOPE * LATENT * heads,
    )

    def more(early, state):
        keys = sum(s.shape[1] for s in early)
        return call(
            functools.partial(attend, heads, len(early), state is None),
            state_shape,
            1,
            (span_ids, queries, *early) + (() if state is None else state),
            2 * total_rows * keys * (2 * LATENT + ROPE),
            [pltpu.VMEM((width, keys), jnp.bfloat16)],
        )

    if (outer_n, inner_n) == (4, 2):
        odd = lambda i: i & core
        near = lambda i: i ^ (1 if odd(i) else step)
        far = lambda i: i ^ (step if odd(i) else 1)
        pair = lambda a: swap(a, TOKENS, n, lambda i: i ^ core)
        first = swap(own, TOKENS, n, near)
        second = swap(own, TOKENS, n, far)
        third = swap(own, TOKENS, n, lambda i: i ^ (step + 1))
        early = [own, pair(own), first, second, pair(first), pair(second)]
        late = [third, pair(third)]
        state = more(early, None)
    else:
        everything = lax.all_gather(own, TOKENS, axis=1, tiled=True)
        chunk = 8 * rows
        blocks = everything.shape[1] // chunk
        piece = lambda i: lax.dynamic_slice_in_dim(everything, i * chunk, chunk, 1)
        state = lax.fori_loop(1, blocks, lambda i, s: more([piece(i)], s), more([piece(0)], None))
        late = [everything[:, (n - 1) * rows :]]
        if blocks == 1:
            raise NotImplementedError("one block")
    me = lax.axis_index("head")
    where = me ^ jnp.arange(head_n, dtype=jnp.int32)
    block = jax.ShapeDtypeStruct((rows, out_proj.shape[1] // head_n), jnp.bfloat16)
    keys = sum(s.shape[1] for s in late)
    parts = call(
        functools.partial(finish, heads, len(late), head_n),
        tuple(block for _ in range(head_n)),
        2,
        (span_ids, where, queries, *late, *state, value_up, out_proj),
        2 * total_rows * keys * (2 * LATENT + ROPE),
        [pltpu.VMEM((width, keys), jnp.bfloat16), pltpu.VMEM((rows, heads * VDIM), jnp.bfloat16)],
    )
    arrived = [
        swap(parts[k], "head", head_n, lambda i: i ^ k) for k in range(head_n - 1, 0, -1)
    ]
    return call(add_parts, block, 0, (parts[0], *arrived), 1 << 18)


def solution(mesh):
    sizes = tuple(mesh.shape[a] for a in ("head", "outer", "inner"))
    return jax.shard_map(
        functools.partial(shards, sizes),
        mesh=mesh,
        in_specs=(
            P(("outer", "inner"), "head"),
            P(("outer", "inner"), "head"),
            P(("outer", "inner"), None),
            P(("outer", "inner")),
            P(None, "head"),
            P(None, "head"),
            P("head", None),
        ),
        out_specs=P(("outer", "inner"), "head"),
        check_vma=False,
    )
```

```python
import functools

import jax
import jax.numpy as jnp
from jax import lax
from jax.experimental import pallas as pl
from jax.experimental.pallas import tpu as pltpu
from jax.sharding import PartitionSpec as P


LATENT = 512
ROPE = 64
NOPE = 128
VDIM = 128
SPAN = 64
TAG = 16

lowest_start = -1e30
log2e = 1.4426950408889634
soft_scale = (NOPE + ROPE) ** (-0.5)
VMEM_BYTES = 24 * 1024 * 1024
NT = (((1,), (1,)), ((), ()))
TOKENS = ("outer", "inner")


def call(body, out_shape, args, flops, scratch=(), spaces=pltpu.VMEM):
    if spaces == pltpu.HBM:
        args = [pltpu.with_memory_space_constraint(a, pltpu.HBM) for a in args]
    return pl.pallas_call(
        body,
        out_shape=out_shape,
        in_specs=[pl.BlockSpec(memory_space=spaces)] * len(args),
        out_specs=jax.tree.map(lambda _: pl.BlockSpec(memory_space=pltpu.VMEM), out_shape),
        scratch_shapes=list(scratch),
        compiler_params=pltpu.CompilerParams(vmem_limit_bytes=VMEM_BYTES),
        cost_estimate=pl.CostEstimate(flops=flops, bytes_accessed=1 << 20, transcendentals=0),
    )(*args)


def prepare(ids_ref, cache_ref, out_ref, ids, sems):
    rows = cache_ref.shape[1]
    keys_in = pltpu.make_async_copy(cache_ref, out_ref.at[: LATENT + ROPE, :], sems.at[0])
    ids_in = pltpu.make_async_copy(ids_ref, ids, sems.at[1])
    keys_in.start()
    ids_in.start()
    ids_in.wait()
    lane = lax.broadcasted_iota(jnp.int32, (TAG, rows), 1)
    tag = jnp.zeros((TAG, rows), jnp.int32)
    for k in range(rows // SPAN):
        tag = jnp.where(lane // SPAN == k, ids[k], tag)
    out_ref[LATENT + ROPE :, :] = tag.astype(jnp.float32).astype(jnp.bfloat16)
    keys_in.wait()


def build_queries(heads, *refs):
    _, _, _, _, out_ref, pos_ref = refs[:6]
    key_up_ref, nope_ref, rope_ref, ids, sems = refs[6:]
    rows = nope_ref.shape[0]
    pairs = zip(refs[:4], refs[6:10])
    loads = [pltpu.make_async_copy(src, dst, sems.at[k]) for k, (src, dst) in enumerate(pairs)]
    for load in loads:
        load.start()
    for load in loads:
        load.wait()
    for h in range(heads):
        here = slice(h * rows, (h + 1) * rows)
        latent = lax.dot_general(
            nope_ref[:, h * NOPE : (h + 1) * NOPE],
            key_up_ref[:, h * NOPE : (h + 1) * NOPE],
            NT,
            preferred_element_type=jnp.float32,
        )
        out_ref[here, :LATENT] = latent.astype(jnp.bfloat16)
        out_ref[here, LATENT : LATENT + ROPE] = rope_ref[:, h * ROPE : (h + 1) * ROPE]
    row = lax.broadcasted_iota(jnp.int32, pos_ref.shape, 0) % rows
    pos = row % SPAN
    for k in range(rows // SPAN):
        pos = pos + jnp.where(row // SPAN == k, ids[k] * SPAN, 0)
    pos_ref[...] = pos.astype(jnp.float32)


def gather_keys(shards, keys):
    at = 0
    for ref in shards:
        keys[:, at : at + ref.shape[1]] = ref[...]
        at += ref.shape[1]


def scores_of(q_ref, pos_ref, keys):
    width = keys.shape[1]
    s = jnp.dot(q_ref[...], keys[: LATENT + ROPE, :], preferred_element_type=jnp.float32)
    tag = keys[LATENT + ROPE : LATENT + ROPE + TAG, :][:1].astype(jnp.float32)
    lane = lax.broadcasted_iota(jnp.int32, (1, width), 1) % SPAN
    key_pos = tag * SPAN + lane.astype(jnp.float32)
    return jnp.where(key_pos <= pos_ref[:, :1], s, -jnp.inf)


def weigh(s, m, keys):
    w = jnp.exp2((s - m) * (soft_scale * log2e))
    acc = lax.dot_general(
        w.astype(jnp.bfloat16), keys[:LATENT, :], NT, preferred_element_type=jnp.float32
    )
    return jnp.sum(w, axis=1, keepdims=True), acc


def attend(n_shards, first, q_ref, pos_ref, *refs):
    shards = refs[:n_shards]
    if first:
        m_ref, l_ref, acc_ref, keys = refs[n_shards:]
    else:
        m_in, l_in, acc_in, m_ref, l_ref, acc_ref, keys = refs[n_shards:]
    gather_keys(shards, keys)
    s = scores_of(q_ref, pos_ref, keys)
    old = lowest_start if first else m_in[:, :1]
    m = jnp.maximum(jnp.max(s, axis=1, keepdims=True), old)
    l, acc = weigh(s, m, keys)
    if not first:
        again = jnp.exp2((old - m) * (soft_scale * log2e))
        l = l + l_in[:, :1] * again
        acc = acc + acc_in[...] * again
    m_ref[...] = jnp.broadcast_to(m, m_ref.shape)
    l_ref[...] = jnp.broadcast_to(l, l_ref.shape)
    acc_ref[...] = acc


def finish(heads, n_shards, parts, q_ref, pos_ref, *refs):
    shards = refs[:n_shards]
    m_in, l_in, acc_in, value_ref, proj_ref = refs[n_shards : n_shards + 5]
    outs = refs[n_shards + 5 : n_shards + 5 + parts]
    keys, head_out = refs[n_shards + 5 + parts :]
    rows = q_ref.shape[0] // heads
    gather_keys(shards, keys)
    s = scores_of(q_ref, pos_ref, keys)
    old = m_in[:, :1]
    m = jnp.maximum(jnp.max(s, axis=1, keepdims=True), old)
    l, acc = weigh(s, m, keys)
    again = jnp.exp2((old - m) * (soft_scale * log2e))
    l = l + l_in[:, :1] * again
    latent = ((acc + acc_in[...] * again) * (1.0 / l)).astype(jnp.bfloat16)
    for h in range(heads):
        head_out[:, h * VDIM : (h + 1) * VDIM] = jnp.dot(
            latent[h * rows : (h + 1) * rows],
            value_ref[:, h * VDIM : (h + 1) * VDIM],
            preferred_element_type=jnp.float32,
        ).astype(jnp.bfloat16)
    width = proj_ref.shape[1] // parts
    me = lax.axis_index("head")
    odd = lax.axis_index("outer") % 2
    flips = [(0, 0), (3, 1), (1, 3), (2, 2)] if parts == 4 else [(k, k) for k in range(parts)]
    for out, (even_flip, odd_flip) in zip(outs, flips):
        dest = me ^ (even_flip + odd * (odd_flip - even_flip))
        at = pl.multiple_of(dest * width, 128)
        out[...] = jnp.dot(
            head_out[...], proj_ref[:, pl.ds(at, width)], preferred_element_type=jnp.float32
        ).astype(out.dtype)


def add_parts(*refs):
    total = refs[0][...].astype(jnp.float32)
    for ref in refs[1:-1]:
        total = total + ref[...].astype(jnp.float32)
    refs[-1][...] = total.astype(jnp.bfloat16)


def swap(a, axes, n, flip):
    return lax.ppermute(a, axes, [(i, flip(i)) for i in range(n)])


def shards(sizes, query_nope, query_rope, cache, span_ids, key_up, value_up, out_proj):
    head_n, outer_n, inner_n = sizes
    rows = cache.shape[0]
    heads = key_up.shape[1] // NOPE
    total_rows = heads * rows
    bf16, f32 = jnp.bfloat16, jnp.float32
    width = LATENT + ROPE + TAG
    n = outer_n * inner_n
    core, step = inner_n, 2 * inner_n
    state_shape = (
        jax.ShapeDtypeStruct((total_rows, 128), f32),
        jax.ShapeDtypeStruct((total_rows, 128), f32),
        jax.ShapeDtypeStruct((total_rows, LATENT), f32),
    )
    own = call(
        prepare,
        jax.ShapeDtypeStruct((width, rows), bf16),
        (span_ids, cache.T),
        1 << 20,
        [pltpu.SMEM(span_ids.shape, jnp.int32), pltpu.SemaphoreType.DMA((2,))],
        pltpu.HBM,
    )
    queries, row_pos = call(
        functools.partial(build_queries, heads),
        (
            jax.ShapeDtypeStruct((total_rows, LATENT + ROPE), bf16),
            jax.ShapeDtypeStruct((total_rows, 128), f32),
        ),
        (key_up, query_nope, query_rope, span_ids),
        2 * rows * NOPE * LATENT * heads,
        [pltpu.VMEM(a.shape, a.dtype) for a in (key_up, query_nope, query_rope)]
        + [pltpu.SMEM(span_ids.shape, jnp.int32), pltpu.SemaphoreType.DMA((4,))],
        pltpu.HBM,
    )

    def more(early, state):
        keys = sum(s.shape[1] for s in early)
        return call(
            functools.partial(attend, len(early), state is None),
            state_shape,
            (queries, row_pos, *early) + (() if state is None else tuple(state)),
            2 * total_rows * keys * (2 * LATENT + ROPE),
            [pltpu.VMEM((width, keys), bf16)],
        )

    if (outer_n, inner_n) == (4, 2):
        odd = lambda i: i & core
        near = lambda i: i ^ (1 if odd(i) else step)
        far = lambda i: i ^ (step if odd(i) else 1)
        pair = lambda a: swap(a, TOKENS, n, lambda i: i ^ core)
        first = swap(own, TOKENS, n, near)
        second = swap(own, TOKENS, n, far)
        third = swap(own, TOKENS, n, lambda i: i ^ (step + 1))
        other = pair(own)
        first_pair = pair(first)
        state = more([own, other, first, first_pair], None)
        late = [second, third, pair(second), pair(third)]
    else:
        everything = lax.all_gather(own, TOKENS, axis=1, tiled=True)
        chunk = 8 * rows
        piece = lambda i: lax.dynamic_slice_in_dim(everything, i * chunk, chunk, 1)
        state = more([piece(0)], None)
        last = n // 8 - 1
        state = lax.fori_loop(1, last, lambda i, s: more([piece(i)], s), state)
        late = [everything[:, last * chunk :]]
    block = jax.ShapeDtypeStruct((rows, out_proj.shape[1] // head_n), bf16)
    keys = sum(s.shape[1] for s in late)
    parts = call(
        functools.partial(finish, heads, len(late), head_n),
        tuple(block for _ in range(head_n)),
        (queries, row_pos, *late, *state, value_up, out_proj),
        2 * total_rows * keys * (2 * LATENT + ROPE),
        [pltpu.VMEM((width, keys), bf16), pltpu.VMEM((rows, heads * VDIM), bf16)],
    )
    if head_n == 4:
        mesh_axes = ("head", "outer", "inner")

        def ring(a, even_flip, odd_flip):
            def to(i):
                odd = (i // inner_n) % 2
                return i ^ ((odd_flip if odd else even_flip) * n)

            return swap(a, mesh_axes, head_n * n, to)

        relayed = ring(parts[3], 3, 1)
        straight = ring(parts[1], 3, 1)
        onward = ring((parts[2].astype(f32) + relayed.astype(f32)).astype(bf16), 1, 3)
        arrived = [straight, onward]
    else:
        arrived = [swap(parts[k], "head", head_n, lambda i: i ^ k) for k in range(1, head_n)]
    return call(add_parts, block, (parts[0], *arrived), 1 << 18)


def solution(mesh):
    sizes = tuple(mesh.shape[a] for a in ("head", "outer", "inner"))

    def body(*args):
        return shards(sizes, *args)

    return jax.shard_map(
        body,
        mesh=mesh,
        in_specs=(
            P(("outer", "inner"), "head"),
            P(("outer", "inner"), "head"),
            P(("outer", "inner"), None),
            P(("outer", "inner")),
            P(None, "head"),
            P(None, "head"),
            P("head", None),
        ),
        out_specs=P(("outer", "inner"), "head"),
        check_vma=False,
    )
```
